32 devices in a mesh: first: 8 (over z, core), second: 4 (over y, x).
Axes of the slice: x: 2, y: 2, z: 4, core: 2. Of those that a mesh axis runs over, the one named last changes fastest.
Arguments:
- pair_rows: bfloat16 [96, 96, 128], P('first', 'second'), may hold values from -6 to 6
- in_gain: float32 [128], replicated, may hold values from 0.25 to 1.75
- left_weight: bfloat16 [128, 128], replicated, may hold values from -0.5 to 0.5
- right_weight: bfloat16 [128, 128], replicated, may hold values from -0.5 to 0.5
- mid_gain: float32 [128], replicated, may hold values from 0.25 to 1.75
- out_weight: bfloat16 [128, 128], replicated, may hold values from -0.5 to 0.5
- out_gate: bfloat16 [128, 128], replicated, may hold values from -0.5 to 0.5
Outputs:
- triangle_out: bfloat16 [96, 96, 128], P('first', 'second')
The draws below stay inside these ranges and needn't reach their ends.
All inputs are finite; a program needn't handle non-finite values.
Results may differ from the reference program's by a relative error of at most 0.012.
Values may be sent and summed in bfloat16 or wider, within the bound.
A program may use at most 64 MiB of HBM per device.

```python
import jax
import jax.numpy as jnp
from jax import lax

RESIDUES = 96
PAIR_WIDTH = 128
MIX_WIDTH = 128


def steps_of(stream_key, dims, cuts, smallest, top_value):
    def one(position, shards_of):
        draws = jax.random.uniform(jax.random.fold_in(jax.random.fold_in(stream_key, 6), position), (shards_of,), jnp.float32, smallest / len(cuts), top_value / len(cuts))
        return jnp.repeat(jnp.exp(draws), dims[position] // shards_of).reshape((-1,) + (1,) * (len(dims) - position - 1))

    level = one(*cuts[0])
    for cut in cuts[1:]:
        level = level * one(*cut)
    return level


def gaussian(stream_key, dims, spread, limit, cuts=(), held_as=jnp.bfloat16):
    values = spread * jax.random.normal(stream_key, dims, jnp.float32)
    if cuts:
        values = values * steps_of(stream_key, dims, cuts, -0.22, 0.18)
    return jnp.clip(values, -limit, limit).astype(held_as)


def setup_inputs(seed: int = 0) -> dict:
    key_list = jax.random.split(jax.random.key(seed), 8)
    pair_rows = gaussian(key_list[0], (RESIDUES, RESIDUES, PAIR_WIDTH), 1.0, 6.0, ((0, 8), (1, 4)))
    in_gain = jnp.clip(1.0 + 0.15 * jax.random.normal(key_list[1], (PAIR_WIDTH,), jnp.float32), 0.25, 1.75)
    left_weight = gaussian(key_list[2], (PAIR_WIDTH, MIX_WIDTH), PAIR_WIDTH ** -0.5, 0.5)
    right_weight = gaussian(key_list[3], (PAIR_WIDTH, MIX_WIDTH), PAIR_WIDTH ** -0.5, 0.5)
    mid_gain = jnp.clip(1.0 + 0.15 * jax.random.normal(key_list[4], (MIX_WIDTH,), jnp.float32), 0.25, 1.75)
    out_weight = gaussian(key_list[5], (MIX_WIDTH, PAIR_WIDTH), MIX_WIDTH ** -0.5, 0.5)
    out_gate = gaussian(key_list[6], (PAIR_WIDTH, PAIR_WIDTH), PAIR_WIDTH ** -0.5, 0.5)
    return {"pair_rows": pair_rows, "in_gain": in_gain, "left_weight": left_weight, "right_weight": right_weight, "mid_gain": mid_gain, "out_weight": out_weight, "out_gate": out_gate}


def norm_channels(values, channel_gain):
    centred = values - lax.optimization_barrier(jnp.mean(values, axis=-1, keepdims=True))
    return centred * lax.rsqrt(lax.optimization_barrier(jnp.mean(centred * centred, axis=-1, keepdims=True)) + 1e-05) * channel_gain

def project_pair(pair_in, in_gain, left_weight, right_weight):
    ready = norm_channels(pair_in.astype(jnp.float32), in_gain).astype(jnp.bfloat16)
    ready = lax.optimization_barrier(ready)
    left = jnp.einsum('ijc,cd->ijd', ready.astype(jnp.float32), left_weight.astype(jnp.float32))
    right = jnp.einsum('ijc,cd->ijd', ready.astype(jnp.float32), right_weight.astype(jnp.float32))
    return (ready, left.astype(jnp.bfloat16), right.astype(jnp.bfloat16))

def to_pair(mixed, ready, mid_gain, out_weight, out_gate):
    scaled = norm_channels(mixed.astype(jnp.float32), mid_gain).astype(jnp.bfloat16)
    scaled = lax.optimization_barrier(scaled)
    gate = jax.nn.sigmoid(jnp.einsum('ijc,cd->ijd', ready.astype(jnp.float32), out_gate.astype(jnp.float32)))
    return (jnp.einsum('ijd,dc->ijc', scaled.astype(jnp.float32), out_weight.astype(jnp.float32)) * gate).astype(jnp.bfloat16)

def reference(pair_rows, in_gain, left_weight, right_weight, mid_gain, out_weight, out_gate):
    ready, left, right = project_pair(pair_rows, in_gain, left_weight, right_weight)
    left, right = lax.optimization_barrier((left, right))

    def one_channel(pair_of):
        return (jnp.dot(pair_of[0].T, pair_of[1], preferred_element_type=jnp.float32) * RESIDUES ** (-0.5)).astype(jnp.bfloat16)
    mixed = jnp.moveaxis(lax.map(one_channel, (jnp.moveaxis(left, -1, 0), jnp.moveaxis(right, -1, 0))), 0, -1)
    mixed = lax.optimization_barrier(mixed)
    return to_pair(mixed, ready, mid_gain, out_weight, out_gate)
```

```python
import functools

import jax
import jax.numpy as jnp
from jax import lax
from jax.experimental import pallas as pl
from jax.experimental.pallas import tpu as pltpu
from jax.sharding import PartitionSpec as P

MESH = pl.DeviceIdType.MESH


def norm_channels(values, channel_gain):
    centred = values - jnp.mean(values, axis=-1, keepdims=True)
    return (
        centred
        * lax.rsqrt(jnp.mean(centred * centred, axis=-1, keepdims=True) + 1e-05)
        * channel_gain
    )


def flip(index, bits, count):
    out, weight = 0, 1
    while weight < count:
        out = out + weight * lax.rem(lax.div(index, weight) + (bits // weight) % 2, 2)
        weight *= 2
    return out


def dot(a, b):
    return jnp.dot(a, b, preferred_element_type=jnp.float32)


def triangle_kernel(
    rows, cols, planes, lines,
    x_ref, in_gain_ref, left_w_ref, right_w_ref, mid_gain_ref, out_w_ref, gate_w_ref,
    out_ref,
    split, lsend, lrecv, rsend, rrecv, left32, right32, own, psend, precv, gate,
    lsend_sem, lrecv_sem, rsend_sem, rrecv_sem, psend_sem, precv_sem,
):
    first, second = lax.axis_index("first"), lax.axis_index("second")
    z, core = lax.div(first, 2), lax.rem(first, 2)
    pairs = rows * cols
    half = cols // 2

    def device(z_at, core_at, second_at):
        return {"first": 2 * z_at + core_at, "second": second_at}

    barrier = pltpu.get_barrier_semaphore()
    peers = 0
    for t in range(lines):
        for rel in range(2):
            if t or rel:
                to = device(z, lax.rem(core + rel, 2), flip(second, t, lines))
                pl.semaphore_signal(barrier, inc=1, device_id=to, device_id_type=MESH)
                peers += 1
    for dz in range(1, planes):
        to = device(lax.rem(z + dz, planes), core, second)
        pl.semaphore_signal(barrier, inc=1, device_id=to, device_id_type=MESH)
        peers += 1

    ready = norm_channels(x_ref[...].astype(jnp.float32), in_gain_ref[...]).astype(jnp.bfloat16)
    left = dot(ready, left_w_ref[...])
    for k in range(rows):
        for h in range(2):
            at = k * cols + h * half
            split[h, k * half : (k + 1) * half, :] = left[at : at + half, :]
    for h in range(2):
        lsend[h] = split[h].astype(jnp.bfloat16)
    right = dot(ready, right_w_ref[...]).astype(jnp.bfloat16)
    rsend[...] = right

    pl.semaphore_wait(barrier, peers)

    left_copies = {}
    for t in range(lines - 1, -1, -1):
        for rel in range(2):
            if t or rel:
                to_core = lax.rem(core + rel, 2)
                copy = pltpu.make_async_remote_copy(
                    src_ref=lsend.at[to_core],
                    dst_ref=lrecv.at[t, rel],
                    send_sem=lsend_sem.at[t, rel],
                    recv_sem=lrecv_sem.at[t, rel],
                    device_id=device(z, to_core, flip(second, t, lines)),
                    device_id_type=MESH,
                )
                copy.start()
                left_copies[t, rel] = copy
    right_copy = pltpu.make_async_remote_copy(
        src_ref=rsend,
        dst_ref=rrecv,
        send_sem=rsend_sem,
        recv_sem=rrecv_sem,
        device_id=device(z, 1 - core, second),
        device_id_type=MESH,
    )
    right_copy.start()

    gate[...] = jax.nn.sigmoid(dot(ready, gate_w_ref[...]))
    right32[0] = right.astype(jnp.float32)
    right_copy.wait_recv()
    right32[1] = rrecv[...].astype(jnp.float32)

    part_copies = []
    for t in range(lines):
        for rel in range(2):
            if t or rel:
                left_copies[t, rel].wait_recv()
                left32[rel] = lrecv[t, rel].astype(jnp.float32)
            else:
                left32[rel] = lsend[core].astype(jnp.float32)

        sums = tuple(jnp.zeros((cols, x_ref.shape[1]), jnp.float32) for _ in range(half))
        for rel in range(2):

            def body(k, sums):
                r = right32[rel, pl.ds(pl.multiple_of(k * cols, 8), cols), :]
                return tuple(
                    total + left32[rel, pl.ds(k * half + i, 1), :] * r
                    for i, total in enumerate(sums)
                )

            sums = lax.fori_loop(0, rows, body, sums)

        z_to = flip(second, t, lines)
        is_own = z_to == z

        @pl.when(is_own)
        def _():
            for i, total in enumerate(sums):
                own[i * cols : (i + 1) * cols, :] = total

        for i in range(0, half, 2):
            two = jnp.concatenate([sums[i], sums[i + 1]], axis=0)
            psend[t, i * cols : (i + 2) * cols, :] = two.astype(jnp.bfloat16)
        slot = lax.rem(z - z_to + 2 * planes - 1, planes)
        copy = pltpu.make_async_remote_copy(
            src_ref=psend.at[t],
            dst_ref=precv.at[slot],
            send_sem=psend_sem.at[t],
            recv_sem=precv_sem.at[slot],
            device_id=device(z_to, core, second),
            device_id_type=MESH,
        )
        part_copies.append((is_own, copy))

        @pl.when(jnp.logical_not(is_own))
        def _():
            copy.start()

    total = own[...]
    for slot in range(planes - 1):
        pltpu.make_async_remote_copy(
            src_ref=psend.at[0],
            dst_ref=precv.at[slot],
            send_sem=psend_sem.at[0],
            recv_sem=precv_sem.at[slot],
            device_id=device(lax.rem(z + 1, planes), core, second),
            device_id_type=MESH,
        ).wait_recv()
        total = total + precv[slot].astype(jnp.float32)
    count = rows * 2 * planes
    mixed = (total * count ** (-0.5)).astype(jnp.bfloat16)
    scaled = norm_channels(mixed.astype(jnp.float32), mid_gain_ref[...]).astype(jnp.bfloat16)
    out_ref[...] = (dot(scaled, out_w_ref[...]) * gate[...]).astype(jnp.bfloat16)

    for copy in left_copies.values():
        copy.wait_send()
    right_copy.wait_send()
    for is_own, copy in part_copies:

        @pl.when(jnp.logical_not(is_own))
        def _():
            copy.wait_send()


def triangle(planes, lines, pair_rows, in_gain, left_weight, right_weight, mid_gain, out_weight, out_gate):
    rows, cols, width = pair_rows.shape
    mix = left_weight.shape[1]
    pairs, half = rows * cols, cols // 2
    vmem = pl.BlockSpec(memory_space=pltpu.VMEM)
    bf16, f32 = jnp.bfloat16, jnp.float32
    out = pl.pallas_call(
        functools.partial(triangle_kernel, rows, cols, planes, lines),
        out_shape=jax.ShapeDtypeStruct((pairs, width), bf16),
        in_specs=[vmem] * 7,
        out_specs=vmem,
        scratch_shapes=[
            pltpu.VMEM((2, rows * half, mix), f32),
            pltpu.VMEM((2, rows * half, mix), bf16),
            pltpu.VMEM((lines, 2, rows * half, mix), bf16),
            pltpu.VMEM((pairs, mix), bf16),
            pltpu.VMEM((pairs, mix), bf16),
            pltpu.VMEM((2, rows * half, mix), f32),
            pltpu.VMEM((2, pairs, mix), f32),
            pltpu.VMEM((half * cols, mix), f32),
            pltpu.VMEM((lines, half * cols, mix), bf16),
            pltpu.VMEM((planes - 1, half * cols, mix), bf16),
            pltpu.VMEM((pairs, width), f32),
            pltpu.SemaphoreType.DMA((lines, 2)),
            pltpu.SemaphoreType.DMA((lines, 2)),
            pltpu.SemaphoreType.DMA,
            pltpu.SemaphoreType.DMA,
            pltpu.SemaphoreType.DMA((lines,)),
            pltpu.SemaphoreType.DMA((planes - 1,)),
        ],
        compiler_params=pltpu.CompilerParams(collective_id=0, has_side_effects=True),
    )(
        pair_rows.reshape(pairs, width), in_gain.reshape(1, width), left_weight, right_weight,
        mid_gain.reshape(1, mix), out_weight, out_gate,
    )
    return out.reshape(rows, cols, width)


def shards(pair_rows, in_gain, left_weight, right_weight, mid_gain, out_weight, out_gate):
    ready = norm_channels(pair_rows.astype(jnp.float32), in_gain).astype(jnp.bfloat16)
    ready = lax.optimization_barrier(ready)
    left = jnp.einsum("ijc,cd->ijd", ready, left_weight, preferred_element_type=jnp.float32)
    right = jnp.einsum("ijc,cd->ijd", ready, right_weight, preferred_element_type=jnp.float32)
    left, right = left.astype(jnp.bfloat16), right.astype(jnp.bfloat16)
    count = pair_rows.shape[0] * lax.axis_size("first")
    left_lines, right_lines = (
        lax.all_to_all(left, "first", split_axis=2, concat_axis=0, tiled=True),
        lax.all_to_all(right, "first", split_axis=2, concat_axis=0, tiled=True),
    )
    strip = jnp.einsum(
        "kid,kjd->ijd",
        lax.all_gather(left_lines, "second", axis=1, tiled=True),
        right_lines,
        preferred_element_type=jnp.float32,
    )
    strip = (strip * count ** (-0.5)).astype(jnp.bfloat16)
    mixed = lax.all_to_all(strip, "first", split_axis=0, concat_axis=2, tiled=True)
    scaled = norm_channels(mixed.astype(jnp.float32), mid_gain).astype(jnp.bfloat16)
    scaled = lax.optimization_barrier(scaled)
    gate = jax.nn.sigmoid(
        jnp.einsum("ijc,cd->ijd", ready, out_gate, preferred_element_type=jnp.float32)
    )
    return (
        jnp.einsum("ijd,dc->ijc", scaled, out_weight, preferred_element_type=jnp.float32) * gate
    ).astype(jnp.bfloat16)


def solution(mesh):
    in_specs = (P("first", "second", None), P(), P(), P(), P(), P(), P())
    out_specs = P("first", "second", None)
    planes, lines = mesh.shape["first"] // 2, mesh.shape["second"]
    if mesh.shape["first"] == 2 * lines and lines & (lines - 1) == 0:
        body = functools.partial(triangle, planes, lines)
    else:
        body = shards
    return jax.shard_map(body, mesh=mesh, in_specs=in_specs, out_specs=out_specs, check_vma=False)
```
